32 devices in a mesh: dp: 4 (over z), tensor: 8 (over y, x, core).
Axes of the slice: x: 2, y: 2, z: 4, core: 2. Of those that a mesh axis runs over, the one named last changes fastest.
Arguments:
- tokens: bfloat16 [1024, 4096], P(('dp', 'tensor')), may hold values from -4 to 4
- lengths: int32 [4], replicated, may hold values from 64 to 256, as said below
- norm_gains: float32 [2, 4096], replicated, may hold values from 0.25 to 1.75
- query_weight: bfloat16 [2, 4096, 4096], P(None, None, 'tensor'), may hold values from -0.09375 to 0.09375
- key_weight: bfloat16 [2, 4096, 1024], P(None, None, 'tensor'), may hold values from -0.09375 to 0.09375
- value_weight: bfloat16 [2, 4096, 1024], P(None, None, 'tensor'), may hold values from -0.09375 to 0.09375
- out_weight: bfloat16 [2, 4096, 4096], P(None, 'tensor'), may hold values from -0.09375 to 0.09375
- query_probe: bfloat16 [2, 4096, 4096], P(None, 'dp', 'tensor'), may hold values from -0.09375 to 0.09375
- key_probe: bfloat16 [2, 4096, 1024], P(None, 'dp', 'tensor'), may hold values from -0.09375 to 0.09375
- value_probe: bfloat16 [2, 4096, 1024], P(None, 'dp', 'tensor'), may hold values from -0.09375 to 0.09375
- out_probe: bfloat16 [2, 4096, 4096], P(None, 'tensor', 'dp'), may hold values from -0.09375 to 0.09375
Outputs:
- query_product: float32 [2, 4096, 4096], P(None, 'dp', 'tensor')
- key_product: float32 [2, 4096, 1024], P(None, 'dp', 'tensor')
- value_product: float32 [2, 4096, 1024], P(None, 'dp', 'tensor')
- out_product: float32 [2, 4096, 4096], P(None, 'tensor', 'dp')
The draws below stay inside these ranges and needn't reach their ends.
Inputs may be any that keep to these rules, and one draw needn't show every extreme that they name: lengths[i] counts the leading valid positions of sequence i; the last sequence is full.
All inputs are finite; a program needn't handle non-finite values.
Results may differ from the reference program's by a relative error of at most 0.035.
Values may be sent and summed in bfloat16 or wider, within the bound.
A program may use at most 128 MiB of HBM per device.

```python
import math
import jax
import jax.numpy as jnp
from jax import lax

D = 4096
HEADS = 32
KVH = 8
HD = 128
LAYERS = 2
LEN = 256
SEQUENCES = 4
TOKENS = 1024
N_DP = 4
N_TENSOR = 8


def draw_tokens(key, part):
    keys = jax.random.split(key, 3)
    row_scale = jnp.exp(jax.random.uniform(keys[1], (TOKENS, 1), jnp.float32, 0.0, math.log(10.0)))
    column_scale = jnp.exp(jax.random.uniform(keys[2], (1, D), jnp.float32, 0.0, math.log(10.0)))
    base = jax.random.truncated_normal(keys[0], -4.0, 4.0, (TOKENS, D), jnp.float32)
    return (0.01 * base * row_scale * column_scale).astype(jnp.bfloat16)


def draw_lengths(key, part):
    number = jnp.arange(SEQUENCES)
    lowest = LEN // 4 + LEN // 2 * number // max(SEQUENCES - 1, 1)
    extra = jax.random.randint(key, (SEQUENCES,), 0, LEN // 4 + 1)
    drawn = jnp.minimum(lowest + extra, LEN)
    return jnp.where(number == SEQUENCES - 1, LEN, drawn).astype(jnp.int32)


def block_scale(stream_key, extent, cuts, smallest, high):
    def one(axis_at, shards_of):
        draws = jax.random.uniform(jax.random.fold_in(jax.random.fold_in(stream_key, 6), axis_at), (shards_of,), jnp.float32, smallest / len(cuts), high / len(cuts))
        return jnp.repeat(jnp.exp(draws), extent[axis_at] // shards_of).reshape((-1,) + (1,) * (len(extent) - axis_at - 1))

    level = one(*cuts[0])
    for cut in cuts[1:]:
        level = level * one(*cut)
    return level


def scatter_about(rng, shape, deviation, reach, cuts=(), kind=jnp.bfloat16):
    gain = block_scale(rng, shape, cuts, -0.22, 0.18) if cuts else 1.0
    values = jax.random.normal(rng, shape, jnp.float32) * deviation * gain
    return jnp.minimum(jnp.maximum(values, -reach), reach).astype(kind)


def setup_inputs(seed: int = 0) -> dict:
    seeds = jax.random.split(jax.random.key(seed), 12)
    tokens = draw_tokens(jax.random.fold_in(seeds[11], 71), 0)
    lengths = draw_lengths(jax.random.fold_in(seeds[11], 71), 0)
    norm_gains = jnp.clip(1.0 + 0.15 * jax.random.normal(seeds[2], (LAYERS, D), jnp.float32), 0.25, 1.75)
    query_weight = scatter_about(seeds[3], (LAYERS, D, HEADS * HD), D ** -0.5, 0.09375, ((2, 8),))
    key_weight = scatter_about(seeds[4], (LAYERS, D, KVH * HD), D ** -0.5, 0.09375, ((2, 8),))
    value_weight = scatter_about(seeds[5], (LAYERS, D, KVH * HD), D ** -0.5, 0.09375, ((2, 8),))
    out_weight = scatter_about(seeds[6], (LAYERS, HEADS * HD, D), (HEADS * HD) ** -0.5, 0.09375, ((1, 8),))
    query_probe = scatter_about(seeds[7], (LAYERS, D, HEADS * HD), D ** -0.5, 0.09375, ((1, 4), (2, 8)))
    key_probe = scatter_about(seeds[8], (LAYERS, D, KVH * HD), D ** -0.5, 0.09375, ((1, 4), (2, 8)))
    value_probe = scatter_about(seeds[9], (LAYERS, D, KVH * HD), D ** -0.5, 0.09375, ((1, 4), (2, 8)))
    out_probe = scatter_about(seeds[10], (LAYERS, HEADS * HD, D), (HEADS * HD) ** -0.5, 0.09375, ((1, 8), (2, 4)))
    return dict(tokens=tokens, lengths=lengths, norm_gains=norm_gains, query_weight=query_weight, key_weight=key_weight, value_weight=value_weight, out_weight=out_weight, query_probe=query_probe, key_probe=key_probe, value_probe=value_probe, out_probe=out_probe)


EPS = 1e-05
THETA = 500000.0

def multiply(pattern, left_side, right_side):
    return jnp.einsum(pattern, left_side.astype(jnp.float32), right_side.astype(jnp.float32))

def matmul(left_side, right_side):
    return jnp.dot(left_side, right_side, preferred_element_type=jnp.float32)

def rope_tables(length, head_size):
    position = jnp.arange(length).astype(jnp.float32)
    column = jnp.arange(head_size // 2).astype(jnp.float32)
    frequency = jnp.exp(-math.log(THETA) * 2.0 * column / head_size)
    angles = position[:, None] * frequency[None, :]
    return (jnp.cos(angles), jnp.sin(angles))

def rotate(values, cosine_table, sine_table, direction):
    middle = values.shape[-1] // 2
    leading = values[..., :middle]
    trailing = values[..., middle:]
    cosine = cosine_table[None, :, None, :]
    sine_part = direction * sine_table[None, :, None, :]
    return jnp.concatenate([leading * cosine - trailing * sine_part, trailing * cosine + leading * sine_part], axis=-1)

def allowed_mask(size, length):
    row_index = jnp.arange(size)[:, None]
    column_index = jnp.arange(size)[None, :]
    return (column_index <= row_index) & (column_index < length)

def attend(queries, key_heads, value_heads, tangent_queries, tangent_keys, tangent_values, length):
    repeat = queries.shape[1] // key_heads.shape[1]
    key_heads = jnp.repeat(key_heads, repeat, axis=1)
    value_heads = jnp.repeat(value_heads, repeat, axis=1)
    tangent_keys = jnp.repeat(tangent_keys, repeat, axis=1)
    tangent_values = jnp.repeat(tangent_values, repeat, axis=1)
    scaling = 1.0 / math.sqrt(queries.shape[-1])
    allowed = allowed_mask(queries.shape[0], length)[None]
    scores = multiply('ihd,jhd->hij', queries, key_heads) * scaling
    powers = jnp.where(allowed, jnp.exp(scores), 0.0)
    weights = powers / lax.optimization_barrier(jnp.sum(powers, axis=-1, keepdims=True))
    weights_low = weights.astype(jnp.bfloat16)
    blended = multiply('hij,jhd->ihd', weights_low, value_heads).astype(jnp.bfloat16)
    tangent_scores = (multiply('ihd,jhd->hij', tangent_queries, key_heads) + multiply('ihd,jhd->hij', queries, tangent_keys)) * scaling
    tangent_weights = weights * (tangent_scores - lax.optimization_barrier(jnp.sum(weights * tangent_scores, axis=-1, keepdims=True)))
    tangent_blended = multiply('hij,jhd->ihd', tangent_weights.astype(jnp.bfloat16), value_heads) + multiply('hij,jhd->ihd', weights_low, tangent_values)
    return (blended, tangent_blended.astype(jnp.bfloat16))

def attend_back(queries, key_heads, value_heads, grad_mixed, length):
    repeat = queries.shape[1] // key_heads.shape[1]
    key_heads = jnp.repeat(key_heads, repeat, axis=1)
    value_heads = jnp.repeat(value_heads, repeat, axis=1)
    scaling = 1.0 / math.sqrt(queries.shape[-1])
    allowed = allowed_mask(queries.shape[0], length)[None]
    scores = multiply('ihd,jhd->hij', queries, key_heads) * scaling
    powers = jnp.where(allowed, jnp.exp(scores), 0.0)
    weights = powers / lax.optimization_barrier(jnp.sum(powers, axis=-1, keepdims=True))
    weights_low = weights.astype(jnp.bfloat16)
    grad_weights = multiply('ihd,jhd->hij', grad_mixed, value_heads)
    grad_values = multiply('hij,ihd->jhd', weights_low, grad_mixed)
    grad_scores = (weights * (grad_weights - lax.optimization_barrier(jnp.sum(weights * grad_weights, axis=-1, keepdims=True))) * scaling).astype(jnp.bfloat16)
    grad_queries = multiply('hij,jhd->ihd', grad_scores, key_heads)
    grad_keys = multiply('hij,ihd->jhd', grad_scores, queries)
    return (grad_queries, grad_keys, grad_values)

def normalize(stream, gain_row):
    wide_stream = stream.astype(jnp.float32)
    inverse = lax.rsqrt(lax.optimization_barrier(jnp.mean(wide_stream * wide_stream, axis=-1, keepdims=True)) + EPS)
    return (wide_stream, inverse, (wide_stream * inverse * gain_row).astype(jnp.bfloat16))

def norm_tangent(wide_stream, inverse, tangent, gain_row):
    shift = lax.optimization_barrier(jnp.mean(wide_stream * tangent, axis=-1, keepdims=True))
    return (gain_row * (tangent * inverse - wide_stream * inverse * inverse * inverse * shift)).astype(jnp.bfloat16)

def norm_back(wide_stream, inverse, grad_normed, gain_row):
    scaled = grad_normed * gain_row
    shift = lax.optimization_barrier(jnp.mean(wide_stream * scaled, axis=-1, keepdims=True))
    return inverse * (scaled - wide_stream * inverse * inverse * shift)

def device_sum(left_terms, right_terms):

    def accumulate(running, pieces):
        partial_value = jnp.zeros_like(running)
        for left_side, right_side in zip(pieces[0], pieces[1]):
            partial_value = partial_value + matmul(left_side, right_side)
        return (running + lax.optimization_barrier(partial_value.astype(jnp.bfloat16)).astype(jnp.float32), None)
    start = jnp.zeros((left_terms[0].shape[1], right_terms[0].shape[2]), jnp.float32)
    running, unused = lax.scan(accumulate, start, (left_terms, right_terms))
    return running

def group_sum(function, arrays, shape):
    batches = tuple((member.reshape((N_DP, member.shape[0] // N_DP) + member.shape[1:]) for member in arrays))

    def accumulate(running, pieces):
        partial_value = function(*pieces)
        return (running + lax.optimization_barrier(partial_value.astype(jnp.bfloat16)).astype(jnp.float32), None)
    running, unused = lax.scan(accumulate, jnp.zeros(shape, jnp.float32), batches)
    return running

def transpose_product(left_side, right_side):
    return matmul(left_side.T, right_side)

def head_pairs(normed_piece, key_piece):
    per_group = multiply('td,tnc->ndc', normed_piece, key_piece)
    group_size = N_TENSOR // KVH
    summed = per_group.reshape(KVH, group_size, per_group.shape[1], per_group.shape[2]).sum(axis=1)
    return summed.transpose(1, 0, 2).reshape(per_group.shape[1], -1)

def reference(tokens, lengths, norm_gains, query_weight, key_weight, value_weight, out_weight, query_probe, key_probe, value_probe, out_probe):
    group_size = N_TENSOR // KVH
    per_device = HEADS // N_TENSOR
    cosine_table, sine_table = rope_tables(LEN, HD)
    token_count = lengths.shape[0] * LEN
    position = jnp.arange(token_count) % LEN
    row_mask = (position < jnp.repeat(lengths, LEN)).astype(jnp.float32)

    def heads_of(values, count):
        return values.reshape(-1, LEN, count, HD)

    def flatten(values):
        return values.reshape(token_count, -1)

    def split_devices(values, columns):
        return values.reshape(token_count, N_TENSOR, columns).transpose(1, 0, 2)
    stream = tokens
    tangent = None
    stored = []
    for layer_index in range(LAYERS):
        gain_row = norm_gains[layer_index].astype(jnp.float32)
        wide_stream, inverse, normed = normalize(stream, gain_row)
        query_primal = matmul(normed, query_weight[layer_index])
        key_primal = matmul(normed, key_weight[layer_index])
        value_primal = matmul(normed, value_weight[layer_index])
        query_moved = matmul(normed, query_probe[layer_index])
        key_moved = matmul(normed, key_probe[layer_index])
        value_moved = matmul(normed, value_probe[layer_index])
        if tangent is not None:
            tangent_normed = norm_tangent(wide_stream, inverse, tangent, gain_row)
            query_moved = query_moved + matmul(tangent_normed, query_weight[layer_index])
            key_moved = key_moved + matmul(tangent_normed, key_weight[layer_index])
            value_moved = value_moved + matmul(tangent_normed, value_weight[layer_index])
        queries = rotate(heads_of(query_primal, HEADS), cosine_table, sine_table, 1.0).astype(jnp.bfloat16)
        key_heads = rotate(heads_of(key_primal, KVH), cosine_table, sine_table, 1.0).astype(jnp.bfloat16)
        value_heads = heads_of(value_primal, KVH).astype(jnp.bfloat16)
        tangent_queries = rotate(heads_of(query_moved, HEADS), cosine_table, sine_table, 1.0).astype(jnp.bfloat16)
        tangent_keys = rotate(heads_of(key_moved, KVH), cosine_table, sine_table, 1.0).astype(jnp.bfloat16)
        tangent_values = heads_of(value_moved, KVH).astype(jnp.bfloat16)
        blended, tangent_blended = lax.map(lambda pieces: attend(*pieces), (queries, key_heads, value_heads, tangent_queries, tangent_keys, tangent_values, lengths))
        blended = flatten(blended)
        tangent_blended = flatten(tangent_blended)
        out_split = out_weight[layer_index].reshape(N_TENSOR, per_device * HD, D)
        probe_split = out_probe[layer_index].reshape(N_TENSOR, per_device * HD, D)
        blended_split = split_devices(blended, per_device * HD)
        tangent_out = device_sum((split_devices(tangent_blended, per_device * HD), blended_split), (out_split, probe_split))
        stored.append((wide_stream, inverse, normed, queries, key_heads, value_heads, blended))
        if layer_index < LAYERS - 1:
            primal_out = device_sum((blended_split,), (out_split,))
            stream = (wide_stream + primal_out).astype(jnp.bfloat16)
        tangent = tangent_out if tangent is None else tangent + tangent_out
    cotangent = row_mask[:, None] * tangent
    query_products = [None] * LAYERS
    key_products = [None] * LAYERS
    value_products = [None] * LAYERS
    out_products = [None] * LAYERS
    for layer_index in reversed(range(LAYERS)):
        wide_stream, inverse, normed, queries, key_heads, value_heads, blended = stored[layer_index]
        cotangent_low = cotangent.astype(jnp.bfloat16)
        out_products[layer_index] = group_sum(transpose_product, (blended, cotangent_low), (HEADS * HD, D))
        grad_mixed = matmul(cotangent_low, out_weight[layer_index].T).astype(jnp.bfloat16)
        grad_queries, grad_keys, grad_values = lax.map(lambda pieces: attend_back(*pieces), (queries, key_heads, value_heads, heads_of(grad_mixed, HEADS), lengths))
        query_low = flatten(rotate(grad_queries, cosine_table, sine_table, -1.0).astype(jnp.bfloat16))
        key_grouped = grad_keys.reshape(-1, LEN, N_TENSOR, per_device, HD).sum(axis=3)
        key_low = rotate(key_grouped, cosine_table, sine_table, -1.0).astype(jnp.bfloat16).reshape(token_count, N_TENSOR, HD)
        value_low = grad_values.reshape(-1, LEN, N_TENSOR, per_device, HD).sum(axis=3).astype(jnp.bfloat16).reshape(token_count, N_TENSOR, HD)
        query_products[layer_index] = group_sum(transpose_product, (normed, query_low), (D, HEADS * HD))
        key_products[layer_index] = group_sum(head_pairs, (normed, key_low), (D, KVH * HD))
        value_products[layer_index] = group_sum(head_pairs, (normed, value_low), (D, KVH * HD))
        if layer_index > 0:
            key_split = jnp.repeat(key_weight[layer_index].reshape(D, KVH, HD).transpose(1, 2, 0), group_size, axis=0)
            value_split = jnp.repeat(value_weight[layer_index].reshape(D, KVH, HD).transpose(1, 2, 0), group_size, axis=0)
            query_split = query_weight[layer_index].T.reshape(N_TENSOR, per_device * HD, D)
            grad_normed = device_sum((split_devices(query_low, per_device * HD), key_low.transpose(1, 0, 2), value_low.transpose(1, 0, 2)), (query_split, key_split, value_split))
            cotangent = cotangent + norm_back(wide_stream, inverse, grad_normed, norm_gains[layer_index].astype(jnp.float32))
    return (jnp.stack(query_products), jnp.stack(key_products), jnp.stack(value_products), jnp.stack(out_products))
```

```python
import math

import jax
import jax.numpy as jnp
from jax import lax
from jax.sharding import PartitionSpec as P

KVH = 8
HD = 128
LEN = 256


EPS = 1e-05
THETA = 500000.0


def swapped(value, axis, apart):
    mask = 2**apart
    pairs = [(source, source ^ mask) for source in range(lax.axis_size(axis))]
    return lax.ppermute(value, axis, pairs)


def matmul(left_side, right_side):
    return jnp.dot(left_side, right_side, preferred_element_type=jnp.float32)


def contract_rows(left_side, right_side):
    return lax.dot_general(
        left_side, right_side, (((0,), (0,)), ((), ())), preferred_element_type=jnp.float32
    )


def contract_last(left_side, right_side):
    return lax.dot_general(
        left_side, right_side, (((1,), (1,)), ((), ())), preferred_element_type=jnp.float32
    )


def rope_tables(length, head_size):
    position = jnp.arange(length).astype(jnp.float32)
    column = jnp.arange(head_size // 2).astype(jnp.float32)
    frequency = jnp.exp(-math.log(THETA) * 2.0 * column / head_size)
    angles = position[:, None] * frequency[None, :]
    return (jnp.cos(angles), jnp.sin(angles))


def rotate(values, cosine_table, sine_table, direction):
    middle = values.shape[-1] // 2
    leading = values[..., :middle]
    trailing = values[..., middle:]
    sine_part = direction * sine_table
    return jnp.concatenate(
        [
            leading * cosine_table - trailing * sine_part,
            trailing * cosine_table + leading * sine_part,
        ],
        axis=-1,
    )


def low(values):
    return values.astype(jnp.bfloat16)


def by_head(values):
    return jnp.transpose(values.reshape(values.shape[0], -1, HD), (1, 0, 2))


def by_token(values, length):
    heads = values.reshape(-1, length, HD)
    return jnp.transpose(heads, (1, 0, 2)).reshape(length, -1)


def softmax_weights(queries, keys, length):
    size = keys.shape[0]
    scores = contract_last(queries, keys) * (1.0 / math.sqrt(HD))
    scores = scores.reshape(-1, size, size)
    row_index = lax.broadcasted_iota(jnp.int32, scores.shape, 1)
    column_index = lax.broadcasted_iota(jnp.int32, scores.shape, 2)
    allowed = (column_index <= row_index) & (column_index < length)
    powers = jnp.where(allowed, jnp.exp(scores), 0.0)
    weights = powers / jnp.sum(powers, axis=-1, keepdims=True)
    return weights.reshape(-1, size)


def centred(weights, values):
    return weights * (values - jnp.sum(weights * values, axis=-1, keepdims=True))


def attend(queries, keys, values, tangent_queries, tangent_keys, tangent_values, length):
    weights = softmax_weights(queries, keys, length)
    weights_low = low(weights)
    blended = low(matmul(weights_low, values))
    tangent_scores = (
        contract_last(tangent_queries, keys) + contract_last(queries, tangent_keys)
    ) * (1.0 / math.sqrt(HD))
    tangent_weights = low(centred(weights, tangent_scores))
    tangent_blended = matmul(tangent_weights, values) + matmul(weights_low, tangent_values)
    return (blended, low(tangent_blended), weights, weights_low)


def attend_back(queries, keys, values, weights, weights_low, grad_mixed):
    grad_weights = contract_last(grad_mixed, values)
    grad_values = contract_rows(weights_low, grad_mixed)
    grad_scores = low(centred(weights, grad_weights) * (1.0 / math.sqrt(HD)))
    return (
        matmul(grad_scores, keys),
        contract_rows(grad_scores, queries),
        grad_values,
    )


def normalize(stream, gain_row):
    inverse = lax.rsqrt(jnp.mean(stream * stream, axis=-1, keepdims=True) + EPS)
    return (inverse, low(stream * inverse * gain_row))


def norm_tangent(stream, inverse, tangent, gain_row):
    shift = jnp.mean(stream * tangent, axis=-1, keepdims=True)
    return low(gain_row * (tangent * inverse - stream * inverse * inverse * inverse * shift))


def norm_back(stream, inverse, grad_normed, gain_row):
    scaled = grad_normed * gain_row
    shift = jnp.mean(stream * scaled, axis=-1, keepdims=True)
    return inverse * (scaled - stream * inverse * inverse * shift)


def body(
    tokens,
    lengths,
    norm_gains,
    query_weight,
    key_weight,
    value_weight,
    out_weight,
    query_probe,
    key_probe,
    value_probe,
    out_probe,
):
    tensor_count = lax.axis_size("tensor")
    tensor_index = lax.axis_index("tensor")
    batches = lax.axis_size("dp")
    data_index = lax.axis_index("dp")
    share_rows = tokens.shape[0]
    group_rows = share_rows * tensor_count
    seq_count = group_rows // LEN
    layer_count = query_weight.shape[0]
    half_width = key_weight.shape[2]
    query_width = query_weight.shape[2]
    block = query_probe.shape[1]
    out_block = out_probe.shape[2]
    cosine_table, sine_table = rope_tables(LEN, HD)
    group_lengths = lax.dynamic_slice_in_dim(lengths, data_index * seq_count, seq_count)
    position = tensor_index * share_rows + jnp.arange(share_rows)
    row_mask = (position % LEN < group_lengths[position // LEN]).astype(jnp.float32)
    lower_half = tensor_index % 2 == 0
    paired = tensor_count > KVH

    def join_halves(own_part):
        if not paired:
            return own_part
        other_part = swapped(own_part, "tensor", 0)
        return jnp.where(
            lower_half,
            jnp.concatenate([own_part, other_part], axis=-1),
            jnp.concatenate([other_part, own_part], axis=-1),
        )

    def split_halves(values):
        if not paired:
            return values
        first, second = (values[:, :half_width], values[:, half_width:])
        own_part = jnp.where(lower_half, first, second)
        other_part = jnp.where(lower_half, second, first)
        received = swapped(other_part, "tensor", 0)
        return low(own_part.astype(jnp.float32) + received.astype(jnp.float32))

    def shifted(values, apart):
        pairs = [(source, (source + apart) % batches) for source in range(batches)]
        return lax.ppermute(values, "dp", pairs)

    def source_of(step):
        return (data_index + batches - step) % batches

    def fetch(values):
        return [values] + [shifted(values, step) for step in range(1, batches)]

    def deal(values, width):
        def chunk(step):
            index = (data_index + step) % batches
            return lax.dynamic_slice_in_dim(values, index * width, width, axis=1)

        return [chunk(0)] + [shifted(chunk(step), step) for step in range(1, batches)]

    def gather(values, axis=0):
        return lax.all_gather(values, "tensor", axis=axis, tiled=True)

    def scatter(values):
        return lax.psum_scatter(
            low(values), "tensor", scatter_dimension=0, tiled=True
        ).astype(jnp.float32)

    def returned_probe(blocks, layer_index):
        rows = blocks.reshape(batches * group_rows, block)
        parts = [
            matmul(rows, probe[layer_index]).reshape(batches, group_rows, -1)
            for probe in (query_probe, key_probe, value_probe)
        ]
        whole = jnp.concatenate(parts, axis=-1)
        total = whole[0]
        for step in range(1, batches):
            total = total + shifted(low(whole[step]), batches - step).astype(jnp.float32)
        return (
            total[:, :query_width],
            total[:, query_width : query_width + half_width],
            total[:, query_width + half_width :],
        )

    def fetched_probe(normed, pieces):
        totals = [0.0, 0.0, 0.0]
        for step in range(batches):
            columns = lax.dynamic_slice_in_dim(normed, source_of(step) * block, block, axis=1)
            for number in range(3):
                totals[number] = totals[number] + matmul(columns, pieces[number][step])
        return totals

    key_full = [join_halves(key_weight[number]) for number in range(layer_count)]
    value_full = [join_halves(value_weight[number]) for number in range(layer_count)]

    stream = tokens.astype(jnp.float32)
    inverse, normed = normalize(stream, norm_gains[0])
    first_blocks = gather(jnp.stack(deal(normed, block)), axis=1)
    normed_all = gather(normed)
    out_pieces = [fetch(out_probe[0])]
    probe_pieces = [None]
    for layer_index in range(1, layer_count):
        probe_pieces.append(
            [fetch(probe[layer_index]) for probe in (query_probe, key_probe, value_probe)]
        )
        out_pieces.append(fetch(out_probe[layer_index]))

    def heads(values, table_direction):
        grouped = by_head(values)
        if table_direction is not None:
            grouped = rotate(grouped, cosine_table, sine_table, table_direction)
        return low(grouped).reshape(-1, HD)

    tangent = None
    tangent_all = None
    stored = []
    for layer_index in range(layer_count):
        final_layer = layer_index == layer_count - 1
        if layer_index == 0:
            blocks = first_blocks.reshape(batches * group_rows, block)
            moved = list(returned_probe(first_blocks, 0))
        else:
            blocks = jnp.concatenate(deal(normed_all, block), axis=0)
            moved = fetched_probe(normed_all, probe_pieces[layer_index])
        moved = [moved[0], join_halves(moved[1]), join_halves(moved[2])]
        weights_here = (query_weight[layer_index], key_full[layer_index], value_full[layer_index])
        primal = [matmul(normed_all, weight) for weight in weights_here]
        if tangent_all is not None:
            moved = [
                part + matmul(tangent_all, weight) for part, weight in zip(moved, weights_here)
            ]
        kv_count = primal[1].shape[1] // HD
        repeat_width = query_width // kv_count
        kept = {}
        blended_rows = []
        tangent_rows = []
        for seq in range(seq_count):
            rows = slice(seq * LEN, (seq + 1) * LEN)
            blended_columns = []
            tangent_columns = []
            for head in range(kv_count):
                wide = slice(head * repeat_width, (head + 1) * repeat_width)
                narrow = slice(head * HD, (head + 1) * HD)
                queries = heads(primal[0][rows, wide], 1.0)
                keys = heads(primal[1][rows, narrow], 1.0)
                values = heads(primal[2][rows, narrow], None)
                blended, tangent_blended, weights, weights_low = attend(
                    queries,
                    keys,
                    values,
                    heads(moved[0][rows, wide], 1.0),
                    heads(moved[1][rows, narrow], 1.0),
                    heads(moved[2][rows, narrow], None),
                    group_lengths[seq],
                )
                kept[seq, head] = (queries, keys, values, weights, weights_low)
                blended_columns.append(by_token(blended, LEN))
                tangent_columns.append(by_token(tangent_blended, LEN))
            blended_rows.append(jnp.concatenate(blended_columns, axis=1))
            tangent_rows.append(jnp.concatenate(tangent_columns, axis=1))
        blended = jnp.concatenate(blended_rows, axis=0)
        tangent_blended = jnp.concatenate(tangent_rows, axis=0)
        tangent_part = matmul(tangent_blended, out_weight[layer_index])
        for step in range(batches):
            start = source_of(step) * out_block
            piece = matmul(blended, out_pieces[layer_index][step])
            piece = piece + lax.dynamic_slice_in_dim(tangent_part, start, out_block, axis=1)
            tangent_part = lax.dynamic_update_slice_in_dim(tangent_part, piece, start, axis=1)
        stored.append((stream, inverse, blocks, fetch(blended), kept))
        if not final_layer:
            stream = low(stream + scatter(matmul(blended, out_weight[layer_index]))).astype(
                jnp.float32
            )
            inverse, normed = normalize(stream, norm_gains[layer_index + 1])
            normed_all = gather(normed)
        tangent_sum = scatter(tangent_part)
        tangent = tangent_sum if tangent is None else tangent + tangent_sum
        if not final_layer:
            tangent_all = gather(
                norm_tangent(stream, inverse, tangent, norm_gains[layer_index + 1])
            )
    cotangent = row_mask[:, None] * tangent
    collected = [None] * layer_count
    for layer_index in reversed(range(layer_count)):
        stream, inverse, blocks, blended_pieces, kept = stored[layer_index]
        cotangent_all = gather(low(cotangent))
        grad_mixed = low(contract_last(cotangent_all, out_weight[layer_index]))
        cotangent_blocks = deal(cotangent_all, out_block)
        out_product = contract_rows(
            jnp.concatenate(blended_pieces, axis=0), jnp.concatenate(cotangent_blocks, axis=0)
        )
        kv_count = key_full[layer_index].shape[1] // HD
        repeat_width = query_width // kv_count
        parts = ([], [], [])
        for seq in range(seq_count):
            rows = slice(seq * LEN, (seq + 1) * LEN)
            columns = ([], [], [])
            for head in range(kv_count):
                wide = slice(head * repeat_width, (head + 1) * repeat_width)
                mixed = by_head(grad_mixed[rows, wide]).reshape(-1, HD)
                grad_queries, grad_keys, grad_values = attend_back(*kept[seq, head], mixed)
                grad_queries = rotate(
                    grad_queries.reshape(-1, LEN, HD), cosine_table, sine_table, -1.0
                )
                columns[0].append(by_token(low(grad_queries), LEN))
                columns[1].append(low(rotate(grad_keys, cosine_table, sine_table, -1.0)))
                columns[2].append(low(grad_values))
            for number in range(3):
                parts[number].append(jnp.concatenate(columns[number], axis=1))
        query_low, key_low, value_low = [jnp.concatenate(part, axis=0) for part in parts]
        if layer_index > 0:
            grad_part = (
                contract_last(query_low, query_weight[layer_index])
                + contract_last(key_low, key_full[layer_index])
                + contract_last(value_low, value_full[layer_index])
            )
            cotangent = cotangent + norm_back(
                stream, inverse, scatter(grad_part), norm_gains[layer_index]
            )
        sent = jnp.concatenate([query_low, split_halves(key_low), split_halves(value_low)], axis=1)
        product = contract_rows(blocks, jnp.concatenate(fetch(sent), axis=0))
        collected[layer_index] = (
            product[:, :query_width],
            product[:, query_width : query_width + half_width],
            product[:, query_width + half_width :],
            out_product,
        )
    return tuple(
        jnp.stack([collected[number][which] for number in range(layer_count)])
        for which in range(4)
    )


def solution(mesh):
    placed = (
        P(("dp", "tensor"), None),
        P(),
        P(),
        P(None, None, "tensor"),
        P(None, None, "tensor"),
        P(None, None, "tensor"),
        P(None, "tensor", None),
        P(None, "dp", "tensor"),
        P(None, "dp", "tensor"),
        P(None, "dp", "tensor"),
        P(None, "tensor", "dp"),
    )
    return jax.shard_map(
        body,
        mesh=mesh,
        in_specs=placed,
        out_specs=(
            P(None, "dp", "tensor"),
            P(None, "dp", "tensor"),
            P(None, "dp", "tensor"),
            P(None, "tensor", "dp"),
        ),
        check_vma=False,
    )
```
